16 devices in a mesh: dp: 4 (over y, z, core), ep: 4 (over x).
Axes of the slice: x: 4, y: 2, z: 1, core: 2. Of those that a mesh axis runs over, the one named last changes fastest.
The devices are a block of a 4x4x8 slice.
Arguments:
- x: bfloat16 [4, 4, 768, 2048], P('dp', 'ep'), parts along dimension 0
- expert: int32 [4, 4, 768, 6], P('dp', 'ep'), parts along dimension 0
- slot: int32 [4, 4, 768, 6], P('dp', 'ep'), parts along dimension 0
- gate: float32 [4, 4, 768, 6], P('dp', 'ep'), parts along dimension 0
- w_gate: bfloat16 [64, 2048, 1408], P('ep')
- w_up: bfloat16 [64, 2048, 1408], P('ep')
- w_down: bfloat16 [64, 1408, 2048], P('ep')
- s_gate: bfloat16 [2048, 2816], replicated
- s_up: bfloat16 [2048, 2816], replicated
- s_down: bfloat16 [2816, 2048], replicated
Outputs:
- y: bfloat16 [4, 4, 768, 2048], P('dp', 'ep'), parts along dimension 0
There are 4 independent parts. The reference program is written for one: setup_inputs(seed, part) draws one part's arguments, and reference() takes and returns one part's arrays. A program takes and returns all parts, laid end to end along the dimension named above; an argument that names none is the same for every part.
All inputs are finite; a program needn't handle non-finite values.
Results may differ from the reference program's by a relative error of at most 0.009.
Values are sent between devices in bfloat16 or wider.
A program may use at most 768 MiB of HBM per device.

```python
import jax
import jax.numpy as jnp

MEMBERS = 4
TOKENS = 768
D = 2048
FF = 1408
TOP = 6
EXPERTS = 64
SHARED_FF = 2816
SLOTS = 5 * TOKENS * TOP // (4 * EXPERTS)


def setup_inputs(seed: int = 0, part: int = 0) -> dict:
    own, k1, k2, k3, k4, k5, k6 = jax.random.split(jax.random.key(seed), 7)
    kx, ke, kl, kg = jax.random.split(jax.random.fold_in(own, part), 4)
    devices = (1, MEMBERS)
    place = jax.random.permutation(kl, jnp.arange(EXPERTS, dtype=jnp.uint32))
    slow = ((EXPERTS + (9 * place) % EXPERTS) << ((9 * place) // EXPERTS)) // EXPERTS
    wait = (jax.random.bits(ke, (*devices, TOKENS, EXPERTS), jnp.uint32) >> 10) * slow
    expert = jnp.argsort(wait, axis=-1)[..., :TOP].astype(jnp.int32)
    chosen = jax.nn.one_hot(expert, EXPERTS, dtype=jnp.int32)
    in_line = jnp.cumsum(chosen.reshape(*devices, TOKENS * TOP, EXPERTS), axis=2) - 1
    slot = jnp.sum(in_line.reshape(chosen.shape) * chosen, axis=-1)

    def one(key, rows, columns):
        return (jax.random.normal(key, (rows, columns), jnp.float32) * rows**-0.5).astype(jnp.bfloat16)

    def weights(key, rows, columns):
        return jax.lax.map(lambda k: one(k, rows, columns), jax.random.split(key, EXPERTS))

    return {
        "x": jax.random.normal(kx, (*devices, TOKENS, D), jnp.float32).astype(jnp.bfloat16),
        "expert": expert,
        "slot": slot,
        "gate": jax.nn.softmax(jax.random.normal(kg, expert.shape, jnp.float32)),
        "w_gate": weights(k1, D, FF),
        "w_up": weights(k2, D, FF),
        "w_down": weights(k3, FF, D),
        "s_gate": one(k4, D, SHARED_FF),
        "s_up": one(k5, D, SHARED_FF),
        "s_down": one(k6, SHARED_FF, D),
    }


def einsum(form, a, b):
    return jnp.einsum(form, a.astype(jnp.float32), b.astype(jnp.float32))


def for_all(x, s_gate, s_up, s_down):
    h = jax.nn.silu(einsum("...d,df->...f", x, s_gate)) * einsum("...d,df->...f", x, s_up)
    return einsum("...f,fd->...d", h.astype(jnp.bfloat16), s_down)


def reference(x, expert, slot, gate, w_gate, w_up, w_down, s_gate, s_up, s_down):
    to_expert = jax.nn.one_hot(expert, EXPERTS, dtype=jnp.bfloat16)
    to_slot = jax.nn.one_hot(slot, SLOTS, dtype=jnp.bfloat16)
    weighted = to_expert * gate[..., None].astype(jnp.bfloat16)
    dispatch = einsum("abtke,abtkc->abtec", to_expert, to_slot).astype(jnp.bfloat16)
    combine = einsum("abtke,abtkc->abtec", weighted, to_slot).astype(jnp.bfloat16)
    z = einsum("abtec,abtd->aebcd", dispatch, x).astype(jnp.bfloat16)
    h = jax.nn.silu(einsum("aebcd,edf->aebcf", z, w_gate))
    h = (h * einsum("aebcd,edf->aebcf", z, w_up)).astype(jnp.bfloat16)
    out = einsum("aebcf,efd->aebcd", h, w_down).astype(jnp.bfloat16)
    y = einsum("abtec,aebcd->abtd", combine, out)
    return (y + for_all(x, s_gate, s_up, s_down)).astype(jnp.bfloat16)
```

```python
import functools

import jax
import jax.numpy as jnp
from jax import lax
from jax.experimental import pallas as pl
from jax.experimental.pallas import tpu as pltpu
from jax.sharding import PartitionSpec as P


CHUNKS = 4
UNIT = 16
BLOCK = 256
F32, BF16 = jnp.float32, jnp.bfloat16
VMEM_LIMIT = 60 * 1024 * 1024
ANY = pl.BlockSpec(memory_space=pl.ANY)
SMEM = pl.BlockSpec(memory_space=pltpu.SMEM)
VMEM = pl.BlockSpec(memory_space=pltpu.VMEM)


def params(**kw):
    return pltpu.CompilerParams(vmem_limit_bytes=VMEM_LIMIT, **kw)


def cost(flops, bytes_accessed):
    return pl.CostEstimate(flops=int(flops), bytes_accessed=int(bytes_accessed), transcendentals=0)


def column_tiles(width, tile):
    return [(c, min(tile, width - c)) for c in range(0, width, tile)]


def for_tiles(width, tile, body):
    whole = width // tile
    if whole:

        @pl.loop(0, whole)
        def _(i):
            body(pl.multiple_of(i * tile, tile), tile)

    if width % tile:
        body(whole * tile, width % tile)


def build_kernel(n_experts, meta, tab, onehot, comb, hits, weights, stage, hit_sem, comb_sem):
    s = pl.program_id(0)
    padded, tokens = tab.shape[1], hits.shape[1]
    ids = lax.broadcasted_iota(jnp.int32, (padded, tokens), 1).astype(F32)
    for e in range(n_experts):
        rows = pl.ds(pl.multiple_of(meta[4 + s, e] * UNIT, UNIT), padded)
        hit = tab[s, :, e : e + 1] == ids
        hits[rows, :] = jnp.where(hit, 1.0, 0.0).astype(BF16)
        weights[rows, :] = jnp.where(hit, tab[s, :, n_experts + e : n_experts + e + 1], 0.0).astype(BF16)

    total = meta[4 + s, n_experts - 1] + meta[s, n_experts - 1]
    per = BLOCK // UNIT
    blocks = (total + per - 1) // per

    @pl.loop(total, blocks * per)
    def _(u):
        rows = pl.ds(pl.multiple_of(u * UNIT, UNIT), UNIT)
        hits[rows, :] = jnp.zeros((UNIT, tokens), BF16)
        weights[rows, :] = jnp.zeros((UNIT, tokens), BF16)

    def block(b):
        return pl.ds(pl.multiple_of(b * BLOCK, BLOCK), BLOCK)

    def hit_copy(b):
        return pltpu.make_async_copy(hits.at[block(b)], onehot.at[s, b], hit_sem.at[b])

    def comb_copy(b):
        return pltpu.make_async_copy(stage.at[b], comb.at[s, b], comb_sem.at[b])

    @pl.loop(0, blocks)
    def _(b):
        hit_copy(b).start()
        stage[b] = weights[block(b), :].T
        comb_copy(b).start()

    @pl.loop(0, blocks)
    def _(b):
        hit_copy(b).wait()
        comb_copy(b).wait()


def build(meta, tab, tokens, slots_padded):
    n_experts = meta.shape[1]
    rows = n_experts * slots_padded
    blocks = rows // BLOCK
    return pl.pallas_call(
        functools.partial(build_kernel, n_experts),
        grid=(4,),
        out_shape=[
            jax.ShapeDtypeStruct((4, blocks, BLOCK, tokens), BF16),
            jax.ShapeDtypeStruct((4, blocks, tokens, BLOCK), BF16),
        ],
        in_specs=[SMEM, VMEM],
        out_specs=[ANY, ANY],
        scratch_shapes=[
            pltpu.VMEM((rows, tokens), BF16),
            pltpu.VMEM((rows, tokens), BF16),
            pltpu.VMEM((blocks, tokens, BLOCK), BF16),
            pltpu.SemaphoreType.DMA((blocks,)),
            pltpu.SemaphoreType.DMA((blocks,)),
        ],
        compiler_params=params(),
        cost_estimate=cost(1.5e10, 2e7),
        name="build",
    )(meta, tab)


def start_loads(pieces, x, x_sem):
    start, loads = 0, []
    for i, piece in enumerate(pieces):
        rows = piece.shape[0]
        copy = pltpu.make_async_copy(piece, x.at[pl.ds(start, rows)], x_sem.at[i])
        copy.start()
        loads.append(copy)
        start += rows
    return loads


def block_count(meta, s, n_experts):
    total = meta[4 + s, n_experts - 1] + meta[s, n_experts - 1]
    per = BLOCK // UNIT
    return (total + per - 1) // per


def dispatch_kernel(source, n_experts, meta, onehot, *refs):
    *pieces, z, x, hits, stage, x_sem, hit_sem, out_sem = refs
    width = x.shape[1]
    blocks = block_count(meta, source, n_experts)

    def hit_copy(b):
        return pltpu.make_async_copy(onehot.at[source, b], hits.at[b], hit_sem.at[b])

    def out_copy(b):
        rows = pl.ds(pl.multiple_of(b * BLOCK, BLOCK), BLOCK)
        return pltpu.make_async_copy(stage.at[b], z.at[rows], out_sem.at[b])

    loads = start_loads(pieces, x, x_sem)

    @pl.loop(0, blocks)
    def _(b):
        hit_copy(b).start()

    for copy in loads:
        copy.wait()

    @pl.loop(0, blocks)
    def _(b):
        hit_copy(b).wait()
        for c, n in column_tiles(width, 512):
            got = jnp.dot(hits[b], x[:, c : c + n], preferred_element_type=F32)
            stage[b, :, c : c + n] = got.astype(BF16)
        out_copy(b).start()

    @pl.loop(0, blocks)
    def _(b):
        out_copy(b).wait()


def dispatch(source, meta, onehot, pieces):
    n_experts = meta.shape[1]
    width = pieces[0].shape[1]
    _, blocks, _, tokens = onehot.shape
    return pl.pallas_call(
        functools.partial(dispatch_kernel, source, n_experts),
        out_shape=jax.ShapeDtypeStruct((blocks * BLOCK, width), BF16),
        in_specs=[SMEM, ANY] + [ANY] * len(pieces),
        out_specs=ANY,
        scratch_shapes=[
            pltpu.VMEM((tokens, width), BF16),
            pltpu.VMEM((blocks, BLOCK, tokens), BF16),
            pltpu.VMEM((blocks, BLOCK, width), BF16),
            pltpu.SemaphoreType.DMA((len(pieces),)),
            pltpu.SemaphoreType.DMA((blocks,)),
            pltpu.SemaphoreType.DMA((blocks,)),
        ],
        compiler_params=params(),
        cost_estimate=cost(5e9, 8e6),
    )(meta, onehot, *pieces)


def sizes(limit):
    return [m for m in (128, 256) if m < limit] + [limit]


def for_rows(rows, limit, body):
    low = 0
    for m in sizes(limit):
        pl.when((rows > low) & (rows <= m))(functools.partial(body, m))
        low = m


def up_kernel(n_experts, meta, onehot, z0, z1, z2, x_a, x_b, wg, wu, h, *scratch):
    gbuf, ubuf, x, hits, z3, zin, hst, g_sem, u_sem, x_sem, hit_sem, z_sem, h_sem = scratch
    zs = (z0, z1, z2)
    e, n = pl.program_id(0), pl.num_programs(0)
    slot = lax.rem(e, 2)
    deep = gbuf.shape[0]
    width, ff = x.shape[1], hst.shape[1]

    def unit(i):
        return pl.ds(pl.multiple_of(i * UNIT, UNIT), UNIT)

    def weight_copies(e):
        i = lax.rem(e, deep)
        return (
            pltpu.make_async_copy(wg.at[e], gbuf.at[i], g_sem.at[i]),
            pltpu.make_async_copy(wu.at[e], ubuf.at[i], u_sem.at[i]),
        )

    def in_copy(s, base, slot, k):
        return pltpu.make_async_copy(zs[s].at[unit(base)], zin.at[slot, unit(k)], z_sem.at[slot, k])

    def load(e, slot):
        k = 0
        for s in range(3):
            count, base = meta[s, e], meta[4 + s, e]

            @pl.loop(0, count)
            def _(u, s=s, k=k, base=base):
                in_copy(s, base + u, slot, k + u).start()

            k = k + count

    @pl.when(e == 0)
    def _():
        loads = start_loads((x_a, x_b), x, x_sem)
        blocks = block_count(meta, 3, n_experts)

        def hit_copy(b):
            return pltpu.make_async_copy(onehot.at[3, b], hits.at[b], hit_sem.at[b])

        @pl.loop(0, blocks)
        def _(b):
            hit_copy(b).start()

        load(e, slot)
        for i in range(deep):
            for copy in weight_copies(i):
                copy.start(priority=1)
        for copy in loads:
            copy.wait()

        @pl.loop(0, blocks)
        def _(b):
            hit_copy(b).wait()
            rows = pl.ds(pl.multiple_of(b * BLOCK, BLOCK), BLOCK)
            for c, size in column_tiles(width, 512):
                got = jnp.dot(hits[b], x[:, c : c + size], preferred_element_type=F32)
                z3[rows, c : c + size] = got.astype(BF16)

    @pl.when(e + 1 < n)
    def _():
        load(e + 1, 1 - slot)

    total = meta[8, e]
    fourth = total - meta[3, e]

    @pl.loop(0, meta[3, e])
    def _(u):
        zin[slot, unit(fourth + u), :] = z3[unit(meta[7, e] + u), :]

    @pl.loop(0, fourth)
    def _(k):
        in_copy(0, 0, slot, k).wait()

    def out_copy(e, m):
        dst = pl.ds(pl.multiple_of(meta[9, e] * UNIT, UNIT), m)
        return pltpu.make_async_copy(hst.at[pl.ds(0, m)], h.at[dst], h_sem)

    @pl.when(e > 0)
    def _():
        for_rows(meta[8, e - 1] * UNIT, zin.shape[1], lambda m: out_copy(e - 1, m).wait())

    for copy in weight_copies(e):
        copy.wait()
    place = lax.rem(e, deep)

    def compute(m):
        for c, size in column_tiles(ff, 256):
            rows = zin[slot, pl.ds(0, m), :]
            g = jnp.dot(rows, gbuf[place, :, c : c + size], preferred_element_type=F32)
            u = jnp.dot(rows, ubuf[place, :, c : c + size], preferred_element_type=F32)
            hst[pl.ds(0, m), c : c + size] = (jax.nn.silu(g) * u).astype(BF16)
        out_copy(e, m).start()

    for_rows(total * UNIT, zin.shape[1], compute)

    @pl.when(e + deep < n)
    def _():
        for copy in weight_copies(e + deep):
            copy.start(priority=1)

    @pl.when(e + 1 == n)
    def _():
        for_rows(total * UNIT, zin.shape[1], lambda m: out_copy(e, m).wait())


def gate_up(meta, onehot, zs, x_far, w_gate, w_up, slots_padded):
    n_experts, width, ff = w_gate.shape
    most = 4 * slots_padded
    _, blocks, _, tokens = onehot.shape
    deep = min(3, n_experts)
    return pl.pallas_call(
        functools.partial(up_kernel, n_experts),
        grid=(n_experts,),
        out_shape=jax.ShapeDtypeStruct((n_experts * most, ff), BF16),
        in_specs=[SMEM] + [ANY] * 8,
        out_specs=ANY,
        scratch_shapes=[
            pltpu.VMEM((deep, width, ff), BF16),
            pltpu.VMEM((deep, width, ff), BF16),
            pltpu.VMEM((tokens, width), BF16),
            pltpu.VMEM((blocks, BLOCK, tokens), BF16),
            pltpu.VMEM((blocks * BLOCK, width), BF16),
            pltpu.VMEM((2, most, width), BF16),
            pltpu.VMEM((most, ff), BF16),
            pltpu.SemaphoreType.DMA((deep,)),
            pltpu.SemaphoreType.DMA((deep,)),
            pltpu.SemaphoreType.DMA((2,)),
            pltpu.SemaphoreType.DMA((blocks,)),
            pltpu.SemaphoreType.DMA((2, most // UNIT)),
            pltpu.SemaphoreType.DMA,
        ],
        compiler_params=params(dimension_semantics=("arbitrary",)),
        cost_estimate=cost(6e10, 2e8),
        name="gate_up",
    )(meta, onehot, *zs, *x_far, w_gate, w_up)


def down_kernel(n_experts, start, meta, comb, h, wd, own, left_sum, left_send, right_sum, right_send, far_a, far_b, *scratch):
    hin, wbuf, ost, obuf, cbuf, acc, h_sem, w_sem, c_sem = scratch
    e, n = pl.program_id(0), pl.num_programs(0)
    deep = hin.shape[0]
    slot = lax.rem(e, deep)
    most, cols = ost.shape
    tokens = acc.shape[0]
    half = tokens // 2
    per = BLOCK // UNIT

    def unit(i):
        return pl.ds(pl.multiple_of(i * UNIT, UNIT), UNIT)

    def total_units(s):
        return meta[4 + s, n_experts - 1] + meta[s, n_experts - 1]

    def comb_copy(s, b):
        lanes = pl.ds(pl.multiple_of(b * BLOCK, BLOCK), BLOCK)
        return pltpu.make_async_copy(comb.at[s, b], cbuf.at[s, :, lanes], c_sem.at[s, b])

    def in_copy(e, m):
        rows = pl.ds(pl.multiple_of(meta[9, e] * UNIT, UNIT), m)
        i = lax.rem(e, deep)
        return pltpu.make_async_copy(h.at[rows], hin.at[i, pl.ds(0, m)], h_sem.at[i])

    def weight_copy(e):
        i = lax.rem(e, deep)
        return pltpu.make_async_copy(wd.at[e, :, pl.ds(start, cols)], wbuf.at[i], w_sem.at[i])

    def load(e):
        for_rows(meta[8, e] * UNIT, most, lambda m: in_copy(e, m).start())
        weight_copy(e).start()

    @pl.when(e == 0)
    def _():
        for i in range(deep):
            load(jnp.int32(i))
        for s in range(4):

            @pl.loop(0, block_count(meta, s, n_experts))
            def _(b, s=s):
                comb_copy(s, b).start()

    weight_copy(e).wait()

    def compute(m):
        in_copy(e, m).wait()
        for c, size in column_tiles(cols, 256):
            got = jnp.dot(hin[slot, pl.ds(0, m), :], wbuf[slot, :, c : c + size], preferred_element_type=F32)
            ost[pl.ds(0, m), c : c + size] = got.astype(BF16)

    for_rows(meta[8, e] * UNIT, most, compute)

    @pl.when(e + deep < n)
    def _():
        load(e + deep)

    padded = most // 4
    k = 0
    for s in range(4):
        to = pl.ds(pl.multiple_of(meta[4 + s, e] * UNIT, UNIT), padded)
        obuf[s, to, :] = ost[pl.ds(pl.multiple_of(k * UNIT, UNIT), padded), :]
        k = k + meta[s, e]

    @pl.when(e + 1 == n)
    def _():
        @pl.loop(0, 4)
        def _(s):
            blocks = block_count(meta, s, n_experts)

            @pl.loop(total_units(s), blocks * per)
            def _(u):
                obuf[s, unit(u), :] = jnp.zeros((UNIT, cols), BF16)

            @pl.loop(0, blocks)
            def _(b):
                comb_copy(s, b).wait()

            @pl.when(blocks == 0)
            def _():
                acc[...] = jnp.zeros_like(acc)

            for count in range(1, comb.shape[1] + 1):

                @pl.when(blocks == count)
                def _(depth=count * BLOCK):
                    def tile(c, size):
                        acc[:, pl.ds(c, size)] = jnp.dot(
                            cbuf[s, :, :depth], obuf[s, :depth, pl.ds(c, size)], preferred_element_type=F32
                        )

                    for_tiles(cols, 256, tile)

            @pl.when(s == 0)
            def _():
                own[...] = acc[...]

            @pl.when(s == 1)
            def _():
                left_send[...] = acc[pl.ds(0, half), :].astype(BF16)
                left_sum[...] = acc[pl.ds(half, half), :]

            @pl.when(s == 2)
            def _():
                right_sum[...] = acc[pl.ds(0, half), :]
                right_send[...] = acc[pl.ds(half, half), :].astype(BF16)

            @pl.when(s == 3)
            def _():
                far_a[...] = acc[pl.ds(0, half), :].astype(BF16)
                far_b[...] = acc[pl.ds(half, half), :].astype(BF16)


def down_combine(meta, comb, h, w_down, slots_padded, start, cols):
    n_experts, ff, width = w_down.shape
    tokens = comb.shape[2]
    most, rows = 4 * slots_padded, n_experts * slots_padded
    half = tokens // 2
    shapes = ((tokens, F32), (half, F32), (half, BF16), (half, F32), (half, BF16), (half, BF16), (half, BF16))
    deep = min(6, n_experts)
    whole = lambda r: pl.BlockSpec((r, cols), lambda e: (0, 0))
    return pl.pallas_call(
        functools.partial(down_kernel, n_experts, start),
        grid=(n_experts,),
        out_shape=[jax.ShapeDtypeStruct((r, cols), t) for r, t in shapes],
        in_specs=[SMEM, ANY, ANY, ANY],
        out_specs=[whole(r) for r, _ in shapes],
        scratch_shapes=[
            pltpu.VMEM((deep, most, ff), BF16),
            pltpu.VMEM((deep, ff, cols), BF16),
            pltpu.VMEM((most, cols), BF16),
            pltpu.VMEM((4, rows, cols), BF16),
            pltpu.VMEM((4, tokens, rows), BF16),
            pltpu.VMEM((tokens, cols), F32),
            pltpu.SemaphoreType.DMA((deep,)),
            pltpu.SemaphoreType.DMA((deep,)),
            pltpu.SemaphoreType.DMA((4, rows // BLOCK)),
        ],
        compiler_params=params(dimension_semantics=("arbitrary",)),
        cost_estimate=cost(4e10 * cols / width, 1e8 * cols / width),
    )(meta, comb, h, w_down)


def final_kernel(own, shared, l0, l1, r0, r1, *refs):
    y = refs[-1]
    half = l0.shape[0]
    for i, (l, r) in enumerate(((l0, r0), (l1, r1))):
        rows = pl.ds(i * half, half)
        y[rows, :] = (own[rows, :] + shared[rows, :] + l[...].astype(F32) + r[...].astype(F32)).astype(BF16)


def final(own, shared, lefts, rights, y, start):
    tokens, cols = own.shape
    half = tokens // 2
    whole = pl.BlockSpec((tokens, cols), lambda i: (0, 0))
    part = pl.BlockSpec((half, cols), lambda i: (0, 0))
    place = pl.BlockSpec((tokens, cols), lambda i: (0, start // cols))
    before = () if y is None else (y,)
    return pl.pallas_call(
        final_kernel,
        grid=(1,),
        out_shape=jax.ShapeDtypeStruct(shared.shape, BF16),
        in_specs=[whole, place] + [part] * 4 + [ANY] * len(before),
        out_specs=place,
        input_output_aliases={6: 0} if before else {},
        compiler_params=params(),
        cost_estimate=cost(2e9, 8e6),
    )(own, shared, *lefts, *rights, *before)


def solution(mesh):
    ring = mesh.shape["ep"]
    assert ring == 4
    to_right = [(i, (i + 1) % ring) for i in range(ring)]
    to_left = [(i, (i - 1) % ring) for i in range(ring)]
    right = lambda v: lax.ppermute(v, "ep", to_right)
    left = lambda v: lax.ppermute(v, "ep", to_left)

    def tables(codes, n_experts, slots, slots_padded):
        expert, slot, gate = (codes[:, :, i] for i in range(3))
        tokens = expert.shape[2]
        here = expert - (lax.axis_index("ep") * n_experts).astype(F32)
        ids = lax.iota(jnp.int32, tokens)
        values = jnp.stack(
            [
                jnp.ones_like(gate),
                jnp.broadcast_to((ids // 128).astype(F32), gate.shape),
                jnp.broadcast_to((ids % 128).astype(F32), gate.shape),
                gate,
            ],
            axis=-1,
        ).astype(BF16)
        to_expert = (here[..., None] == lax.iota(jnp.int32, n_experts).astype(F32)).astype(BF16)
        lhs = (values[..., :, None] * to_expert[..., None, :]).reshape(*gate.shape, 4 * n_experts)
        cell = lax.iota(jnp.int32, slots_padded)
        to_slot = ((slot[..., None] == cell.astype(F32)) & (cell < slots)).astype(BF16)
        got = jnp.einsum("sjtc,sjtm->scm", to_slot, lhs, preferred_element_type=F32)
        used, high, low, weight = jnp.split(got, 4, axis=-1)
        token = jnp.where(used > 0.5, high * 128 + low, -1.0)
        last = jnp.max(jnp.where(used > 0.5, (cell + 1)[:, None], 0), axis=1)
        units = (last + UNIT - 1) // UNIT
        offset = jnp.cumsum(units, axis=1) - units
        total = jnp.sum(units, axis=0, keepdims=True)
        meta = jnp.concatenate([units, offset, total, jnp.cumsum(total, axis=1) - total]).astype(jnp.int32)
        tab = jnp.concatenate([token, weight], axis=-1)
        return meta, jnp.pad(tab, ((0, 0), (0, 0), (0, 128 - tab.shape[-1])))

    def step(x, expert, slot, gate, w_gate, w_up, w_down, s_gate, s_up, s_down):
        x = x[0, 0]
        tokens, width = x.shape
        top = expert.shape[-1]
        n_experts = w_gate.shape[0]
        slots = 5 * tokens * top // (4 * n_experts * ring)
        slots_padded = -(-slots // UNIT) * UNIT
        half = tokens // 2

        codes = jnp.stack(
            [
                expert[0, 0].astype(F32),
                jnp.minimum(slot[0, 0], slots).astype(F32),
                gate[0, 0].astype(BF16).astype(F32),
            ],
            axis=0,
        )
        codes = codes.transpose(2, 0, 1).astype(BF16)
        code_left, code_right = right(codes), left(codes)
        code_far = lax.ppermute(codes, "ep", [(i, (i + 2) % ring) for i in range(ring)])
        x_a, x_b = x[:half], x[half:]
        left_a, right_b = right(x_a), left(x_b)
        left_b, right_a = right(x_b), left(x_a)
        x_far = (right(left_a), left(right_b))

        codes = jnp.stack([codes, code_left, code_right, code_far]).astype(F32)
        meta, tab = tables(codes, n_experts, slots, slots_padded)

        g = jnp.dot(x, s_gate, preferred_element_type=F32)
        u = jnp.dot(x, s_up, preferred_element_type=F32)
        hidden = (jax.nn.silu(g) * u).astype(BF16)
        shared = jnp.dot(hidden, s_down, preferred_element_type=F32)

        meta, tab, shared = lax.optimization_barrier((meta, tab, shared))
        onehot, comb = build(meta, tab, tokens, slots_padded)
        zs = []
        for i, pieces in enumerate(((x,), (left_a, left_b), (right_a, right_b))):
            zs.append(dispatch(i, meta, onehot, pieces))
        h = gate_up(meta, onehot, zs, x_far, w_gate, w_up, slots_padded)

        y = None
        cols = width // CHUNKS
        for c in range(CHUNKS):
            start = c * cols
            own, left_sum, left_send, right_sum, right_send, far_a, far_b = down_combine(
                meta, comb, h, w_down, slots_padded, start, cols
            )
            from_left, from_right = right(far_a), left(far_b)
            lefts = [None, right(right_send)]
            rights = [left(left_send), None]
            lefts[0] = right((right_sum + from_left.astype(F32)).astype(BF16))
            rights[1] = left((left_sum + from_right.astype(F32)).astype(BF16))
            y = final(own, shared, lefts, rights, y, start)
        return y[None, None]

    token_spec = P("dp", "ep", None, None)
    weight_spec = P("ep", None, None)
    return jax.shard_map(
        step,
        mesh=mesh,
        in_specs=(token_spec,) * 4 + (weight_spec,) * 3 + (P(None, None),) * 3,
        out_specs=token_spec,
        check_vma=False,
    )
```

```python
import functools

import jax
import jax.numpy as jnp
from jax import lax
from jax.experimental import pallas as pl
from jax.experimental.pallas import tpu as pltpu
from jax.sharding import PartitionSpec as P


CHUNKS = (3, 3, 2)
UNIT = 16
BLOCK = 256
F32, BF16 = jnp.float32, jnp.bfloat16
VMEM_LIMIT = 60 * 1024 * 1024
ANY = pl.BlockSpec(memory_space=pl.ANY)
SMEM = pl.BlockSpec(memory_space=pltpu.SMEM)
VMEM = pl.BlockSpec(memory_space=pltpu.VMEM)


def params(**kw):
    return pltpu.CompilerParams(vmem_limit_bytes=VMEM_LIMIT, **kw)


def cost(flops, bytes_accessed):
    return pl.CostEstimate(flops=int(flops), bytes_accessed=int(bytes_accessed), transcendentals=0)


def column_tiles(width, tile):
    return [(c, min(tile, width - c)) for c in range(0, width, tile)]


def for_tiles(width, tile, body):
    whole = width // tile
    if whole:

        @pl.loop(0, whole)
        def _(i):
            body(pl.multiple_of(i * tile, tile), tile)

    if width % tile:
        body(whole * tile, width % tile)


def build_kernel(n_experts, meta, tab, onehot, comb, hits, weights, stage, hit_sem, comb_sem):
    s = pl.program_id(0)
    padded, tokens = tab.shape[1], hits.shape[1]
    ids = lax.broadcasted_iota(jnp.int32, (padded, tokens), 1).astype(F32)
    for e in range(n_experts):
        rows = pl.ds(pl.multiple_of(meta[4 + s, e] * UNIT, UNIT), padded)
        hit = tab[s, :, e : e + 1] == ids
        hits[rows, :] = jnp.where(hit, 1.0, 0.0).astype(BF16)
        weights[rows, :] = jnp.where(hit, tab[s, :, n_experts + e : n_experts + e + 1], 0.0).astype(BF16)

    total = meta[4 + s, n_experts - 1] + meta[s, n_experts - 1]
    per = BLOCK // UNIT
    blocks = (total + per - 1) // per

    @pl.loop(total, blocks * per)
    def _(u):
        rows = pl.ds(pl.multiple_of(u * UNIT, UNIT), UNIT)
        hits[rows, :] = jnp.zeros((UNIT, tokens), BF16)
        weights[rows, :] = jnp.zeros((UNIT, tokens), BF16)

    def block(b):
        return pl.ds(pl.multiple_of(b * BLOCK, BLOCK), BLOCK)

    def hit_copy(b):
        return pltpu.make_async_copy(hits.at[block(b)], onehot.at[s, b], hit_sem.at[b])

    def comb_copy(b):
        return pltpu.make_async_copy(stage.at[b], comb.at[s, b], comb_sem.at[b])

    @pl.loop(0, blocks)
    def _(b):
        hit_copy(b).start()
        stage[b] = weights[block(b), :].T
        comb_copy(b).start()

    @pl.loop(0, blocks)
    def _(b):
        hit_copy(b).wait()
        comb_copy(b).wait()


def build(meta, tab, tokens, slots_padded):
    n_experts = meta.shape[1]
    rows = n_experts * slots_padded
    blocks = rows // BLOCK
    return pl.pallas_call(
        functools.partial(build_kernel, n_experts),
        grid=(4,),
        out_shape=[
            jax.ShapeDtypeStruct((4, blocks, BLOCK, tokens), BF16),
            jax.ShapeDtypeStruct((4, blocks, tokens, BLOCK), BF16),
        ],
        in_specs=[SMEM, VMEM],
        out_specs=[ANY, ANY],
        scratch_shapes=[
            pltpu.VMEM((rows, tokens), BF16),
            pltpu.VMEM((rows, tokens), BF16),
            pltpu.VMEM((blocks, tokens, BLOCK), BF16),
            pltpu.SemaphoreType.DMA((blocks,)),
            pltpu.SemaphoreType.DMA((blocks,)),
        ],
        compiler_params=params(),
        cost_estimate=cost(1.5e10, 2e7),
        name="build",
    )(meta, tab)


def start_loads(pieces, x, x_sem):
    start, loads = 0, []
    for i, piece in enumerate(pieces):
        rows = piece.shape[0]
        copy = pltpu.make_async_copy(piece, x.at[pl.ds(start, rows)], x_sem.at[i])
        copy.start()
        loads.append(copy)
        start += rows
    return loads


def block_count(meta, s, n_experts):
    total = meta[4 + s, n_experts - 1] + meta[s, n_experts - 1]
    per = BLOCK // UNIT
    return (total + per - 1) // per


def dispatch_kernel(source, n_experts, meta, onehot, *refs):
    *pieces, z, x, hits, stage, x_sem, hit_sem, out_sem = refs
    width = x.shape[1]
    blocks = block_count(meta, source, n_experts)

    def hit_copy(b):
        return pltpu.make_async_copy(onehot.at[source, b], hits.at[b], hit_sem.at[b])

    def out_copy(b):
        rows = pl.ds(pl.multiple_of(b * BLOCK, BLOCK), BLOCK)
        return pltpu.make_async_copy(stage.at[b], z.at[rows], out_sem.at[b])

    loads = start_loads(pieces, x, x_sem)

    @pl.loop(0, blocks)
    def _(b):
        hit_copy(b).start()

    for copy in loads:
        copy.wait()

    @pl.loop(0, blocks)
    def _(b):
        hit_copy(b).wait()
        for c, n in column_tiles(width, 512):
            got = jnp.dot(hits[b], x[:, c : c + n], preferred_element_type=F32)
            stage[b, :, c : c + n] = got.astype(BF16)
        out_copy(b).start()

    @pl.loop(0, blocks)
    def _(b):
        out_copy(b).wait()


def dispatch(source, meta, onehot, pieces):
    n_experts = meta.shape[1]
    width = pieces[0].shape[1]
    _, blocks, _, tokens = onehot.shape
    return pl.pallas_call(
        functools.partial(dispatch_kernel, source, n_experts),
        out_shape=jax.ShapeDtypeStruct((blocks * BLOCK, width), BF16),
        in_specs=[SMEM, ANY] + [ANY] * len(pieces),
        out_specs=ANY,
        scratch_shapes=[
            pltpu.VMEM((tokens, width), BF16),
            pltpu.VMEM((blocks, BLOCK, tokens), BF16),
            pltpu.VMEM((blocks, BLOCK, width), BF16),
            pltpu.SemaphoreType.DMA((len(pieces),)),
            pltpu.SemaphoreType.DMA((blocks,)),
            pltpu.SemaphoreType.DMA((blocks,)),
        ],
        compiler_params=params(),
        cost_estimate=cost(5e9, 8e6),
    )(meta, onehot, *pieces)


def sizes(limit):
    return [m for m in (128, 256) if m < limit] + [limit]


def for_rows(rows, limit, body, among=None):
    low = 0
    for m in among or sizes(limit):
        pl.when((rows > low) & (rows <= m))(functools.partial(body, m))
        low = m


def up_kernel(n_experts, meta, onehot, z0, z1, z2, x_a, x_b, wg, wu, h, *scratch):
    gbuf, ubuf, x, hits, z3, zin, hst, g_sem, u_sem, x_sem, hit_sem, z_sem, h_sem = scratch
    zs = (z0, z1, z2)
    e, n = pl.program_id(0), pl.num_programs(0)
    slot = lax.rem(e, 2)
    deep = gbuf.shape[0]
    width, ff = x.shape[1], hst.shape[1]

    def unit(i):
        return pl.ds(pl.multiple_of(i * UNIT, UNIT), UNIT)

    def weight_copies(e):
        i = lax.rem(e, deep)
        return (
            pltpu.make_async_copy(wg.at[e], gbuf.at[i], g_sem.at[i]),
            pltpu.make_async_copy(wu.at[e], ubuf.at[i], u_sem.at[i]),
        )

    def in_copy(s, base, slot, k):
        return pltpu.make_async_copy(zs[s].at[unit(base)], zin.at[slot, unit(k)], z_sem.at[slot, k])

    def load(e, slot):
        k = 0
        for s in range(3):
            count, base = meta[s, e], meta[4 + s, e]

            @pl.loop(0, count)
            def _(u, s=s, k=k, base=base):
                in_copy(s, base + u, slot, k + u).start()

            k = k + count

    @pl.when(e == 0)
    def _():
        loads = start_loads((x_a, x_b), x, x_sem)
        blocks = block_count(meta, 3, n_experts)

        def hit_copy(b):
            return pltpu.make_async_copy(onehot.at[3, b], hits.at[b], hit_sem.at[b])

        @pl.loop(0, blocks)
        def _(b):
            hit_copy(b).start()

        load(e, slot)
        for i in range(deep):
            for copy in weight_copies(i):
                copy.start(priority=1)
        for copy in loads:
            copy.wait()

        @pl.loop(0, blocks)
        def _(b):
            hit_copy(b).wait()
            rows = pl.ds(pl.multiple_of(b * BLOCK, BLOCK), BLOCK)
            for c, size in column_tiles(width, 512):
                got = jnp.dot(hits[b], x[:, c : c + size], preferred_element_type=F32)
                z3[rows, c : c + size] = got.astype(BF16)

    @pl.when(e + 1 < n)
    def _():
        load(e + 1, 1 - slot)

    total = meta[8, e]
    fourth = total - meta[3, e]

    @pl.loop(0, meta[3, e])
    def _(u):
        zin[slot, unit(fourth + u), :] = z3[unit(meta[7, e] + u), :]

    @pl.loop(0, fourth)
    def _(k):
        in_copy(0, 0, slot, k).wait()

    def out_copy(e, m):
        dst = pl.ds(pl.multiple_of(meta[9, e] * UNIT, UNIT), m)
        return pltpu.make_async_copy(hst.at[pl.ds(0, m)], h.at[dst], h_sem)

    @pl.when(e > 0)
    def _():
        for_rows(meta[8, e - 1] * UNIT, zin.shape[1], lambda m: out_copy(e - 1, m).wait())

    for copy in weight_copies(e):
        copy.wait()
    place = lax.rem(e, deep)

    def compute(m):
        for c, size in column_tiles(ff, 256):
            rows = zin[slot, pl.ds(0, m), :]
            g = jnp.dot(rows, gbuf[place, :, c : c + size], preferred_element_type=F32)
            u = jnp.dot(rows, ubuf[place, :, c : c + size], preferred_element_type=F32)
            hst[pl.ds(0, m), c : c + size] = (jax.nn.silu(g) * u).astype(BF16)
        out_copy(e, m).start()

    for_rows(total * UNIT, zin.shape[1], compute)

    @pl.when(e + deep < n)
    def _():
        for copy in weight_copies(e + deep):
            copy.start(priority=1)

    @pl.when(e + 1 == n)
    def _():
        for_rows(total * UNIT, zin.shape[1], lambda m: out_copy(e, m).wait())


def gate_up(meta, onehot, zs, x_far, w_gate, w_up, slots_padded):
    n_experts, width, ff = w_gate.shape
    most = 4 * slots_padded
    _, blocks, _, tokens = onehot.shape
    deep = min(3, n_experts)
    return pl.pallas_call(
        functools.partial(up_kernel, n_experts),
        grid=(n_experts,),
        out_shape=jax.ShapeDtypeStruct((n_experts * most, ff), BF16),
        in_specs=[SMEM] + [ANY] * 8,
        out_specs=ANY,
        scratch_shapes=[
            pltpu.VMEM((deep, width, ff), BF16),
            pltpu.VMEM((deep, width, ff), BF16),
            pltpu.VMEM((tokens, width), BF16),
            pltpu.VMEM((blocks, BLOCK, tokens), BF16),
            pltpu.VMEM((blocks * BLOCK, width), BF16),
            pltpu.VMEM((2, most, width), BF16),
            pltpu.VMEM((most, ff), BF16),
            pltpu.SemaphoreType.DMA((deep,)),
            pltpu.SemaphoreType.DMA((deep,)),
            pltpu.SemaphoreType.DMA((2,)),
            pltpu.SemaphoreType.DMA((blocks,)),
            pltpu.SemaphoreType.DMA((2, most // UNIT)),
            pltpu.SemaphoreType.DMA,
        ],
        compiler_params=params(dimension_semantics=("arbitrary",)),
        cost_estimate=cost(6e10, 2e8),
        name="gate_up",
    )(meta, onehot, *zs, *x_far, w_gate, w_up)


def down_kernel(n_experts, start, meta, comb, h, wd, own, left_sum, left_send, right_sum, right_send, far_a, far_b, *scratch):
    hin, wbuf, ost, obuf, cbuf, acc, h_sem, w_sem, c_sem = scratch
    e, n = pl.program_id(0), pl.num_programs(0)
    deep = hin.shape[0]
    slot = lax.rem(e, deep)
    most, cols = ost.shape
    tokens = acc.shape[0]
    half = tokens // 2
    per = BLOCK // UNIT
    fine = [*range(64, most, 64), most]

    def unit(i):
        return pl.ds(pl.multiple_of(i * UNIT, UNIT), UNIT)

    def total_units(s):
        return meta[4 + s, n_experts - 1] + meta[s, n_experts - 1]

    def comb_copy(s, b):
        lanes = pl.ds(pl.multiple_of(b * BLOCK, BLOCK), BLOCK)
        return pltpu.make_async_copy(comb.at[s, b], cbuf.at[s, :, lanes], c_sem.at[s, b])

    def in_copy(e, m):
        rows = pl.ds(pl.multiple_of(meta[9, e] * UNIT, UNIT), m)
        i = lax.rem(e, deep)
        return pltpu.make_async_copy(h.at[rows], hin.at[i, pl.ds(0, m)], h_sem.at[i])

    def weight_copy(e):
        i = lax.rem(e, deep)
        return pltpu.make_async_copy(wd.at[e, :, pl.ds(start, cols)], wbuf.at[i], w_sem.at[i])

    def load(e):
        for_rows(meta[8, e] * UNIT, most, lambda m: in_copy(e, m).start(), fine)
        weight_copy(e).start()

    @pl.when(e == 0)
    def _():
        for i in range(deep):
            load(jnp.int32(i))
        for s in range(4):

            @pl.loop(0, block_count(meta, s, n_experts))
            def _(b, s=s):
                comb_copy(s, b).start()

    weight_copy(e).wait()

    for_rows(meta[8, e] * UNIT, most, lambda m: in_copy(e, m).wait(), fine)

    def compute(m):
        for c, size in column_tiles(cols, 256):
            got = jnp.dot(hin[slot, pl.ds(0, m), :], wbuf[slot, :, c : c + size], preferred_element_type=F32)
            ost[pl.ds(0, m), c : c + size] = got.astype(BF16)

    for_rows(meta[8, e] * UNIT, most, compute)

    @pl.when(e + deep < n)
    def _():
        load(e + deep)

    padded = most // 4
    k = 0
    for s in range(4):
        to = pl.ds(pl.multiple_of(meta[4 + s, e] * UNIT, UNIT), padded)
        obuf[s, to, :] = ost[pl.ds(pl.multiple_of(k * UNIT, UNIT), padded), :]
        k = k + meta[s, e]

    @pl.when(e + 1 == n)
    def _():
        @pl.loop(0, 4)
        def _(s):
            blocks = block_count(meta, s, n_experts)

            @pl.loop(total_units(s), blocks * per)
            def _(u):
                obuf[s, unit(u), :] = jnp.zeros((UNIT, cols), BF16)

            @pl.loop(0, blocks)
            def _(b):
                comb_copy(s, b).wait()

            @pl.when(blocks == 0)
            def _():
                acc[...] = jnp.zeros_like(acc)

            for count in range(1, comb.shape[1] + 1):

                @pl.when(blocks == count)
                def _(depth=count * BLOCK):
                    def tile(c, size):
                        acc[:, pl.ds(c, size)] = jnp.dot(
                            cbuf[s, :, :depth], obuf[s, :depth, pl.ds(c, size)], preferred_element_type=F32
                        )

                    for_tiles(cols, 256, tile)

            @pl.when(s == 0)
            def _():
                own[...] = acc[...]

            @pl.when(s == 1)
            def _():
                left_send[...] = acc[pl.ds(0, half), :].astype(BF16)
                left_sum[...] = acc[pl.ds(half, half), :]

            @pl.when(s == 2)
            def _():
                right_sum[...] = acc[pl.ds(0, half), :]
                right_send[...] = acc[pl.ds(half, half), :].astype(BF16)

            @pl.when(s == 3)
            def _():
                far_a[...] = acc[pl.ds(0, half), :].astype(BF16)
                far_b[...] = acc[pl.ds(half, half), :].astype(BF16)


def down_combine(meta, comb, h, w_down, slots_padded, start, cols):
    n_experts, ff, width = w_down.shape
    tokens = comb.shape[2]
    most, rows = 4 * slots_padded, n_experts * slots_padded
    half = tokens // 2
    shapes = ((tokens, F32), (half, F32), (half, BF16), (half, F32), (half, BF16), (half, BF16), (half, BF16))
    deep = min(5, n_experts)
    whole = lambda r: pl.BlockSpec((r, cols), lambda e: (0, 0))
    return pl.pallas_call(
        functools.partial(down_kernel, n_experts, start),
        grid=(n_experts,),
        out_shape=[jax.ShapeDtypeStruct((r, cols), t) for r, t in shapes],
        in_specs=[SMEM, ANY, ANY, ANY],
        out_specs=[whole(r) for r, _ in shapes],
        scratch_shapes=[
            pltpu.VMEM((deep, most, ff), BF16),
            pltpu.VMEM((deep, ff, cols), BF16),
            pltpu.VMEM((most, cols), BF16),
            pltpu.VMEM((4, rows, cols), BF16),
            pltpu.VMEM((4, tokens, rows), BF16),
            pltpu.VMEM((tokens, cols), F32),
            pltpu.SemaphoreType.DMA((deep,)),
            pltpu.SemaphoreType.DMA((deep,)),
            pltpu.SemaphoreType.DMA((4, rows // BLOCK)),
        ],
        compiler_params=params(dimension_semantics=("arbitrary",)),
        cost_estimate=cost(4e10 * cols / width, 1e8 * cols / width),
    )(meta, comb, h, w_down)


def final_kernel(own, shared, l0, l1, r0, r1, *refs):
    y = refs[-1]
    half = l0.shape[0]
    for i, (l, r) in enumerate(((l0, r0), (l1, r1))):
        rows = pl.ds(i * half, half)
        y[rows, :] = (own[rows, :] + shared[rows, :] + l[...].astype(F32) + r[...].astype(F32)).astype(BF16)


def final(own, shared, lefts, rights, y, start):
    tokens, cols = own.shape
    half = tokens // 2
    whole = pl.BlockSpec((tokens, cols), lambda i: (0, 0))
    part = pl.BlockSpec((half, cols), lambda i: (0, 0))
    place = pl.BlockSpec((tokens, cols), lambda i: (0, start // cols))
    before = () if y is None else (y,)
    return pl.pallas_call(
        final_kernel,
        grid=(1,),
        out_shape=jax.ShapeDtypeStruct(shared.shape, BF16),
        in_specs=[whole, place] + [part] * 4 + [ANY] * len(before),
        out_specs=place,
        input_output_aliases={6: 0} if before else {},
        compiler_params=params(),
        cost_estimate=cost(2e9, 8e6),
    )(own, shared, *lefts, *rights, *before)


def solution(mesh):
    ring = mesh.shape["ep"]
    assert ring == 4
    to_right = [(i, (i + 1) % ring) for i in range(ring)]
    to_left = [(i, (i - 1) % ring) for i in range(ring)]
    right = lambda v: lax.ppermute(v, "ep", to_right)
    left = lambda v: lax.ppermute(v, "ep", to_left)

    def tables(codes, n_experts, slots, slots_padded):
        expert, slot, gate = (codes[:, :, i] for i in range(3))
        tokens = expert.shape[2]
        here = expert - (lax.axis_index("ep") * n_experts).astype(F32)
        ids = lax.iota(jnp.int32, tokens)
        values = jnp.stack(
            [
                jnp.ones_like(gate),
                jnp.broadcast_to((ids // 128).astype(F32), gate.shape),
                jnp.broadcast_to((ids % 128).astype(F32), gate.shape),
                gate,
            ],
            axis=-1,
        ).astype(BF16)
        to_expert = (here[..., None] == lax.iota(jnp.int32, n_experts).astype(F32)).astype(BF16)
        lhs = (values[..., :, None] * to_expert[..., None, :]).reshape(*gate.shape, 4 * n_experts)
        cell = lax.iota(jnp.int32, slots_padded)
        to_slot = ((slot[..., None] == cell.astype(F32)) & (cell < slots)).astype(BF16)
        got = jnp.einsum("sjtc,sjtm->scm", to_slot, lhs, preferred_element_type=F32)
        used, high, low, weight = jnp.split(got, 4, axis=-1)
        token = jnp.where(used > 0.5, high * 128 + low, -1.0)
        last = jnp.max(jnp.where(used > 0.5, (cell + 1)[:, None], 0), axis=1)
        units = (last + UNIT - 1) // UNIT
        offset = jnp.cumsum(units, axis=1) - units
        total = jnp.sum(units, axis=0, keepdims=True)
        meta = jnp.concatenate([units, offset, total, jnp.cumsum(total, axis=1) - total]).astype(jnp.int32)
        tab = jnp.concatenate([token, weight], axis=-1)
        return meta, jnp.pad(tab, ((0, 0), (0, 0), (0, 128 - tab.shape[-1])))

    def step(x, expert, slot, gate, w_gate, w_up, w_down, s_gate, s_up, s_down):
        x = x[0, 0]
        tokens, width = x.shape
        top = expert.shape[-1]
        n_experts = w_gate.shape[0]
        slots = 5 * tokens * top // (4 * n_experts * ring)
        slots_padded = -(-slots // UNIT) * UNIT
        half = tokens // 2

        codes = jnp.stack(
            [
                expert[0, 0].astype(F32),
                jnp.minimum(slot[0, 0], slots).astype(F32),
                gate[0, 0].astype(BF16).astype(F32),
            ],
            axis=0,
        )
        codes = codes.transpose(2, 0, 1).astype(BF16)
        code_left, code_right = right(codes), left(codes)
        code_far = lax.ppermute(codes, "ep", [(i, (i + 2) % ring) for i in range(ring)])
        x_a, x_b = x[:half], x[half:]
        left_a, right_b = right(x_a), left(x_b)
        left_b, right_a = right(x_b), left(x_a)
        x_far = (right(left_a), left(right_b))

        codes = jnp.stack([codes, code_left, code_right, code_far]).astype(F32)
        meta, tab = tables(codes, n_experts, slots, slots_padded)

        g = jnp.dot(x, s_gate, preferred_element_type=F32)
        u = jnp.dot(x, s_up, preferred_element_type=F32)
        hidden = (jax.nn.silu(g) * u).astype(BF16)
        shared = jnp.dot(hidden, s_down, preferred_element_type=F32)

        onehot, comb = build(meta, tab, tokens, slots_padded)
        zs = []
        for i, pieces in enumerate(((x,), (left_a, left_b), (right_a, right_b))):
            zs.append(dispatch(i, meta, onehot, pieces))
        h = gate_up(meta, onehot, zs, x_far, w_gate, w_up, slots_padded)

        y, start = None, 0
        for eighths in CHUNKS:
            cols = width * eighths // 8
            own, left_sum, left_send, right_sum, right_send, far_a, far_b = down_combine(
                meta, comb, h, w_down, slots_padded, start, cols
            )
            from_left, from_right = right(far_a), left(far_b)
            lefts = [None, right(right_send)]
            rights = [left(left_send), None]
            lefts[0] = right((right_sum + from_left.astype(F32)).astype(BF16))
            rights[1] = left((left_sum + from_right.astype(F32)).astype(BF16))
            y = final(own, shared, lefts, rights, y, start)
            start += cols
        return y[None, None]

    token_spec = P("dp", "ep", None, None)
    weight_spec = P("ep", None, None)
    return jax.shard_map(
        step,
        mesh=mesh,
        in_specs=(token_spec,) * 4 + (weight_spec,) * 3 + (P(None, None),) * 3,
        out_specs=token_spec,
        check_vma=False,
    )
```
